128 devices in a mesh: col: 2 (over core), row: 64 (over z, y, x).
Axes of the slice: x: 4, y: 4, z: 4, core: 2. Of those that a mesh axis runs over, the one named last changes fastest.
Arguments:
- w_gate: float32 [512, 1024], P('row', 'col')
- w_up: float32 [512, 1024], P('row', 'col')
- w_down: float32 [1024, 512], P('row', 'col')
- x_norm: bfloat16 [32768, 512], P(None, 'row')
- x_act: bfloat16 [32768, 1024], P(None, 'row')
- dy_gate: bfloat16 [32768, 1024], P(None, 'col')
- dy_up: bfloat16 [32768, 1024], P(None, 'col')
- dy_down: bfloat16 [32768, 512], P(None, 'col')
- r_gate: float32 [512], P('row')
- c_gate: float32 [1024], P('col')
- r_up: float32 [512], P('row')
- c_up: float32 [1024], P('col')
- r_down: float32 [1024], P('row')
- c_down: float32 [512], P('col')
- hyper_params: float32 [3], replicated
Outputs:
- output 1: float32 [512, 1024], P('row', 'col')
- output 2: float32 [512, 1024], P('row', 'col')
- output 3: float32 [1024, 512], P('row', 'col')
- output 4: float32 [512], P('row')
- output 5: float32 [1024], P('col')
- output 6: float32 [512], P('row')
- output 7: float32 [1024], P('col')
- output 8: float32 [1024], P('row')
- output 9: float32 [512], P('col')
- output 10: bfloat16 [32768, 512], P(None, 'row')
- output 11: bfloat16 [32768, 1024], P(None, 'row')
All inputs are finite; a program needn't handle non-finite values.
Results may differ from the reference program's by a relative error of at most 0.001.
Values are sent between devices in bfloat16 or wider.
A program may use at most 1 GiB of HBM per device.

```python
import jax
import jax.numpy as jnp
from jax import lax

D_MODEL = 512
D_FF = 1024
TOKENS = 32768
EPS_ONE = 1e-30
EPS_TWO = 1e-3
TWO_PI = 6.283185307179586


def smooth_field(key, length, log_scale):
    key_amp, key_phase = jax.random.split(key)
    ampl_k = jax.random.normal(key_amp, (3,), jnp.float32)
    phase_k = jax.random.uniform(key_phase, (3,), jnp.float32, minval=0.0, maxval=TWO_PI)
    position = jnp.arange(length, dtype=jnp.float32) / length
    freq_k = jnp.arange(1, 4, dtype=jnp.float32)
    waves = jnp.cos(TWO_PI * position[:, None] * freq_k[None, :] + phase_k[None, :])
    return jnp.exp(log_scale * jnp.sum(waves * ampl_k[None, :], axis=1) / 1.7)


def draw_weight(key, rows, cols):
    key_z, key_r, key_c = jax.random.split(key, 3)
    noise = jax.random.normal(key_z, (rows, cols), jnp.float32)
    row_prof = smooth_field(key_r, rows, 0.5)
    col_prof = smooth_field(key_c, cols, 0.5)
    return noise * (rows ** -0.5) * row_prof[:, None] * col_prof[None, :]


def draw_tokens(key, cols, scale):
    key_z, key_a, key_b = jax.random.split(key, 3)
    noise = jax.random.normal(key_z, (TOKENS, cols), jnp.float32)
    first_half = (jnp.arange(TOKENS) < TOKENS // 2)[:, None]
    profile = jnp.where(first_half, smooth_field(key_a, cols, 0.8)[None, :], smooth_field(key_b, cols, 0.8)[None, :])
    return (noise * profile * scale).astype(jnp.bfloat16)


def draw_stat(key, length):
    return jax.random.uniform(key, (length,), jnp.float32, minval=0.5, maxval=3.0)


def setup_inputs(seed: int = 0) -> dict:
    keys = jax.random.split(jax.random.key(seed), 15)
    tok_scale = TOKENS ** -0.5
    low_end = jnp.array([0.6, 0.6, 0.15], dtype=jnp.float32)
    span_len = jnp.array([0.25, 0.6, 0.15], dtype=jnp.float32)
    unit_draw = jax.random.uniform(keys[14], (3,), jnp.float32)
    return {
        'w_gate': draw_weight(keys[0], D_MODEL, D_FF),
        'w_up': draw_weight(keys[1], D_MODEL, D_FF),
        'w_down': draw_weight(keys[2], D_FF, D_MODEL),
        'x_norm': draw_tokens(keys[3], D_MODEL, tok_scale),
        'x_act': draw_tokens(keys[4], D_FF, tok_scale),
        'dy_gate': draw_tokens(keys[5], D_FF, 1.0),
        'dy_up': draw_tokens(keys[6], D_FF, 1.0),
        'dy_down': draw_tokens(keys[7], D_MODEL, 1.0),
        'r_gate': draw_stat(keys[8], D_MODEL),
        'c_gate': draw_stat(keys[9], D_FF),
        'r_up': draw_stat(keys[10], D_MODEL),
        'c_up': draw_stat(keys[11], D_FF),
        'r_down': draw_stat(keys[12], D_FF),
        'c_down': draw_stat(keys[13], D_MODEL),
        'hyper_params': low_end + span_len * unit_draw,
    }


def factored_step(w_old, grad_w, r_old, c_old, hyper_params):
    beta_two = hyper_params[0]
    grad_sq = grad_w * grad_w + EPS_ONE
    r_new = beta_two * r_old + (1.0 - beta_two) * jnp.mean(grad_sq, axis=1)
    c_new = beta_two * c_old + (1.0 - beta_two) * jnp.mean(grad_sq, axis=0)
    v_est = r_new[:, None] * c_new[None, :] / jnp.mean(r_new)
    update = grad_w * lax.rsqrt(v_est)
    rms_u = jnp.sqrt(jnp.mean(update * update))
    update_hat = update / jnp.maximum(1.0, rms_u / hyper_params[2])
    step_size = hyper_params[1] * jnp.maximum(EPS_TWO, jnp.sqrt(jnp.mean(w_old * w_old)))
    return w_old - step_size * update_hat, r_new, c_new


def weight_grad(activations, grad_out):
    return jnp.dot(activations.T, grad_out, preferred_element_type=jnp.float32)


def input_grad(grad_out, weight):
    return jnp.dot(grad_out, weight.astype(jnp.bfloat16).T, preferred_element_type=jnp.float32)


def reference(w_gate, w_up, w_down, x_norm, x_act, dy_gate, dy_up, dy_down, r_gate, c_gate, r_up, c_up, r_down, c_down, hyper_params):
    new_gate, r_gate_new, c_gate_new = factored_step(w_gate, weight_grad(x_norm, dy_gate), r_gate, c_gate, hyper_params)
    new_up, r_up_new, c_up_new = factored_step(w_up, weight_grad(x_norm, dy_up), r_up, c_up, hyper_params)
    new_down, r_down_new, c_down_new = factored_step(w_down, weight_grad(x_act, dy_down), r_down, c_down, hyper_params)
    dx_norm = (input_grad(dy_gate, w_gate) + input_grad(dy_up, w_up)).astype(jnp.bfloat16)
    dx_act = input_grad(dy_down, w_down).astype(jnp.bfloat16)
    return (new_gate, new_up, new_down, r_gate_new, c_gate_new, r_up_new, c_up_new, r_down_new, c_down_new, dx_norm, dx_act)
```

```python
import functools

import jax
import jax.numpy as jnp
from jax import lax
from jax.experimental import pallas as pl
from jax.experimental.pallas import tpu as pltpu
from jax.sharding import PartitionSpec as P

EPS_ONE = 1e-30
EPS_TWO = 1e-3
MESH = pl.DeviceIdType.MESH
BF16 = jnp.bfloat16
F32 = jnp.float32


def dot_nt(lhs, rhs):
    return lax.dot_general(lhs, rhs, (((1,), (1,)), ((), ())), preferred_element_type=F32)


def dot_nn(lhs, rhs):
    return lax.dot_general(lhs, rhs, (((1,), (0,)), ((), ())), preferred_element_type=F32)


def to_column(row_ref):
    m = row_ref.shape[1]
    eye = lax.broadcasted_iota(jnp.int32, (m, m), 0) == lax.broadcasted_iota(jnp.int32, (m, m), 1)
    spread = jnp.where(eye, jnp.broadcast_to(row_ref[...], (m, m)), 0.0)
    return jnp.broadcast_to(jnp.sum(spread, axis=1, keepdims=True), (m, 128))


def to_row(column):
    m = column.shape[0]
    eye = lax.broadcasted_iota(jnp.int32, (m, m), 0) == lax.broadcasted_iota(jnp.int32, (m, m), 1)
    return jnp.sum(jnp.where(eye, column[:, :m], 0.0), axis=0, keepdims=True)


def widen(column, n):
    return jnp.concatenate([column] * (n // 128), axis=1)


def step_kernel(
    dims,
    hyper, w_gate, w_up, w_down, xn, xa, dyg, dyu, dyd, r_gate, c_gate, r_up, c_up, r_down, c_down,
    w_gate_o, w_up_o, w_down_o, r_gate_o, c_gate_o, r_up_o, c_up_o, r_down_o, c_down_o, dxn_o, dxa_o,
    dyg_v, dyu_v, dya_v, dyb_v,
    wn_v, wa_v, wb_v, wlg_v, wlu_v,
    xrn, xra, xrb, xln,
    dsn, dsa, dsb, dkn, dka, dkb, drn, dra, drb, fin_n, fin_a, fin_b,
    gpn, gpa, gpb, grn, gra, grb,
    rs_v, rr_v, st_v, sr_v, fs_v, fr_v,
    ldg, ldu, lda, ldb, ldx,
    w_ss, w_rs, x_ss, x_rs, xf_ss, xf_rs, p_ss, p_rs, d_ss, d_rs, o_ss, o_rs, o_ls, f_ss, f_rs,
    g_ss, g_rs, r_ss, r_rs, s_ss, s_rs, e_ss, e_rs,
):
    ring, cores, tokens = dims
    m, nf = w_gate.shape
    ma, nd = w_down.shape
    tq = tokens // ring
    th = tq // 2
    aq = tq // 2
    ah = aq // 2
    ct = min(2048, th)
    n_ct = th // ct
    rows = ring**3

    core = lax.axis_index("col")
    row = lax.axis_index("row")
    partner = {"col": 1 - core}
    here, peers = [], []
    for stride in (1, ring, ring * ring):
        q = lax.rem(lax.div(row, stride), ring)
        here.append(q)
        group = []
        for k in range(1, ring):
            there = lax.rem(q + k, ring)
            group.append((k - 1, there, {"row": row + (there - q) * stride}))
        peers.append(group)

    def remote(src, dst, send, recv, device):
        return pltpu.make_async_remote_copy(
            src_ref=src, dst_ref=dst, send_sem=send, recv_sem=recv, device_id=device, device_id_type=MESH
        )

    def half_of(s):
        return core if s else 1 - core

    bases = (0, 0, tokens // 2)
    shares = (tq, aq, aq)
    halves = (th, ah, ah)

    def token_start(axis, q, h):
        return pl.multiple_of(bases[axis] + q * shares[axis] + h * halves[axis], 128)

    def norm_load(src, dst, sem, s, i):
        start = pl.multiple_of(here[0] * tq + half_of(s) * th + i * ct, 128)
        return pltpu.make_async_copy(src.at[pl.ds(start, ct), :], dst.at[s, pl.ds(i * ct, ct), :], sem.at[s, i])

    def down_load(axis, dst, sem, s):
        start = token_start(axis, here[axis], half_of(s))
        return pltpu.make_async_copy(dyd.at[pl.ds(start, ah), :], dst.at[s], sem.at[s])

    x_src = (xn, xa, xa)
    x_dst = (xrn, xra, xrb)

    def x_piece(axis, q, h):
        return x_src[axis].at[:, pl.ds(token_start(axis, q, h), halves[axis])]

    for s in (0, 1):
        for i in range(n_ct):
            norm_load(dyg, dyg_v, ldg, s, i).start()
            norm_load(dyu, dyu_v, ldu, s, i).start()
        down_load(1, dya_v, lda, s).start()
        down_load(2, dyb_v, ldb, s).start()
    own_x = [
        pltpu.make_async_copy(x_piece(a, here[a], h), x_dst[a].at[h, here[a]], ldx.at[a, h])
        for a in range(3)
        for h in (0, 1)
    ]
    for copy in own_x:
        copy.start()

    wn_v[here[0]] = jnp.concatenate([w_gate[...], w_up[...]], axis=0).astype(BF16)
    wa_v[here[1]] = w_down[...].astype(BF16)
    wb_v[here[2]] = w_down[...].astype(BF16)

    barrier = pltpu.get_barrier_semaphore()
    pl.semaphore_signal(barrier, inc=1, device_id=partner, device_id_type=MESH)
    for group in peers:
        for _, _, device in group:
            pl.semaphore_signal(barrier, inc=1, device_id=device, device_id_type=MESH)
    pl.semaphore_wait(barrier, 1 + 3 * (ring - 1))

    w_bufs = (wn_v, wa_v, wb_v)
    w_sends, x_sends = [], []
    for a in range(3):
        for j, there, device in peers[a]:
            slot = w_bufs[a].at[here[a]]
            w_sends.append(remote(slot, slot, w_ss.at[a, j], w_rs.at[a, j], device))
    for j in range(ring - 1):
        for a in range(3):
            _, there, device = peers[a][j]
            x_sends.append(
                remote(x_piece(a, there, core), x_dst[a].at[core, here[a]], x_ss.at[a, j], x_rs.at[a, j], device)
            )
    for copy in w_sends:
        copy.start()
    for copy in x_sends:
        copy.start()

    beta = hyper[0]
    rho = hyper[1]
    bound = hyper[2]
    rc_g, rc_u, rc_d = to_column(r_gate), to_column(r_up), to_column(r_down)
    w_sq = [jnp.sum(w[...] * w[...]).reshape(1, 1) for w in (w_gate, w_up, w_down)]

    for copy in w_sends:
        copy.wait_recv()
    stacked = [wn_v[p].astype(F32) for p in range(ring)]
    wlg_v[...] = jnp.concatenate([v[:m] for v in stacked], axis=0).astype(BF16)
    wlu_v[...] = jnp.concatenate([v[m:] for v in stacked], axis=0).astype(BF16)

    def dx_norm(s, out):
        @pl.loop(0, n_ct)
        def _(i):
            norm_load(dyg, dyg_v, ldg, s, i).wait()
            norm_load(dyu, dyu_v, ldu, s, i).wait()
            part = pl.ds(pl.multiple_of(i * ct, ct), ct)
            out[:, part] = dot_nt(wlg_v[...], dyg_v[s, part, :]) + dot_nt(wlu_v[...], dyu_v[s, part, :])

    def dx_down(axis, s, dy_v, sem, w_v, out):
        down_load(axis, dy_v, sem, s).wait()
        out[...] = dot_nt(w_v[...].reshape(ring * ma, nd), dy_v[s])

    part_sends = [remote(src, dst, p_ss.at[a], p_rs.at[a], partner) for a, (src, dst) in enumerate(((dsn, drn), (dsa, dra), (dsb, drb)))]
    dx_norm(0, dsn)
    part_sends[0].start()
    dx_down(1, 0, dya_v, lda, wa_v, dsa)
    part_sends[1].start()
    dx_down(2, 0, dyb_v, ldb, wb_v, dsb)
    part_sends[2].start()

    dx_out = (dxn_o, dxa_o, dxa_o)
    fins = (fin_n, fin_a, fin_b)

    def out_piece(axis, q, h):
        return dx_out[axis].at[:, pl.ds(token_start(axis, q, h), halves[axis])]

    dx_sends, own_sends, own_copies = [], [], []
    for a in range(3):
        target = out_piece(a, here[a], core)
        own = fins[a].at[here[a]]
        own_sends.append(remote(own, target, o_ss.at[a], o_rs.at[a], partner))
        own_copies.append(pltpu.make_async_copy(own, target, o_ls.at[a]))
        for j, there, device in peers[a]:
            dx_sends.append(remote(fins[a].at[there], target, d_ss.at[a, j], d_rs.at[a, j], device))

    def finish(a, kept, got):
        part_sends[a].wait_recv()
        total = (kept[...] + got[...]).astype(BF16)
        size = fins[a].shape[1]
        for p in range(ring):
            fins[a][p] = total[p * size : (p + 1) * size]
        for copy in dx_sends[a * (ring - 1) : (a + 1) * (ring - 1)]:
            copy.start()
        own_sends[a].start()
        own_copies[a].start()

    dx_norm(1, dkn)
    finish(0, dkn, drn)
    dx_down(1, 1, dya_v, lda, wa_v, dka)
    finish(1, dka, dra)
    dx_down(2, 1, dyb_v, ldb, wb_v, dkb)
    finish(2, dkb, drb)

    x_forwards = []
    for j in range(ring - 1):
        for a in range(3):
            origin = lax.rem(here[a] + ring - (j + 1), ring)
            slot = x_dst[a].at[core, origin]
            x_forwards.append(remote(slot, slot, xf_ss.at[a, j], xf_rs.at[a, j], partner))
    for got, forward in zip(x_sends, x_forwards, strict=True):
        got.wait_recv()
        forward.start()
    for copy in own_x:
        copy.wait()
    for forward in x_forwards:
        forward.wait_recv()

    for h in (0, 1):
        xln[h] = jnp.concatenate([xrn[h, p].astype(F32) for p in range(ring)], axis=0).astype(BF16)
    grads = []
    for dy_v in (dyg_v, dyu_v):
        grads.append(sum(dot_nn(xln[half_of(s)], dy_v[s]) for s in (0, 1)))
    for p in range(ring):
        gpn[p] = jnp.concatenate([g[p * m : (p + 1) * m] for g in grads], axis=0)
    for x_v, dy_v, out in ((xra, dya_v, gpa), (xrb, dyb_v, gpb)):
        total = sum(dot_nn(x_v[half_of(s)].reshape(ring * ma, ah), dy_v[s]) for s in (0, 1))
        out[...] = total.reshape(ring, ma, nd)
    g_sends = []
    for a, (src, dst) in enumerate(((gpn, grn), (gpa, gra), (gpb, grb))):
        for j, there, device in peers[a]:
            g_sends.append(remote(src.at[there], dst.at[here[a]], g_ss.at[a, j], g_rs.at[a, j], device))
    for copy in g_sends:
        copy.start()
    grn[here[0]] = gpn[here[0]]
    gra[here[1]] = gpa[here[1]]
    grb[here[2]] = gpb[here[2]]

    dx_forwards = []
    for a in range(3):
        for j, _, _ in peers[a]:
            origin = lax.rem(here[a] + ring - (j + 1), ring)
            piece = out_piece(a, origin, core)
            dx_forwards.append(remote(piece, piece, f_ss.at[a, j], f_rs.at[a, j], partner))
    for got, forward in zip(dx_sends, dx_forwards, strict=True):
        got.wait_recv()
        forward.start()

    for copy in g_sends:
        copy.wait_recv()
    g_n = sum(grn[p] for p in range(ring))
    g_g, g_u = g_n[:m], g_n[m:]
    g_d = sum(gra[p] for p in range(ring)) + sum(grb[p] for p in range(ring))
    sq = [g * g for g in (g_g, g_u, g_d)]

    offset = 0
    for v in sq:
        size = v.shape[0]
        rs_v[offset : offset + size, :] = jnp.broadcast_to(jnp.sum(v + EPS_ONE, axis=1, keepdims=True), (size, 128))
        offset += size
    row_swap = remote(rs_v, rr_v, r_ss, r_rs, partner)
    row_swap.start()
    row_swap.wait_recv()
    row_sum = rs_v[...] + rr_v[...]
    r_g = beta * rc_g + (1.0 - beta) * (row_sum[:m] / (cores * nf))
    r_u = beta * rc_u + (1.0 - beta) * (row_sum[m : 2 * m] / (cores * nf))
    r_d = beta * rc_d + (1.0 - beta) * (row_sum[2 * m :] / (cores * nd))
    r_gate_o[...] = to_row(r_g)
    r_up_o[...] = to_row(r_u)
    r_down_o[...] = to_row(r_d)

    wide = [widen(r, v.shape[1]) for r, v in zip((r_g, r_u, r_d), sq, strict=True)]
    st_v[...] = jnp.zeros_like(st_v)
    for i in (0, 1):
        st_v[0, 2 * i : 2 * i + 1, :] = jnp.sum(sq[i] + EPS_ONE, axis=0, keepdims=True)
        st_v[0, 2 * i + 1 : 2 * i + 2, :] = jnp.sum(sq[i] / wide[i], axis=0, keepdims=True)
    st_v[0, 4:5, :nd] = jnp.sum(sq[2] + EPS_ONE, axis=0, keepdims=True)
    st_v[0, 4:5, nd:] = jnp.sum(sq[2] / wide[2], axis=0, keepdims=True)
    for i, r in enumerate((r_g, r_u, r_d)):
        st_v[0, 5:6, i * 128 : (i + 1) * 128] = jnp.sum(r, axis=0, keepdims=True)
        st_v[0, 6:7, i * 128 : (i + 1) * 128] = jnp.broadcast_to(w_sq[i], (1, 128))
    stat_sends = []
    for a in range(3):
        sends = [
            remote(st_v.at[a], sr_v.at[a, here[a]], s_ss.at[a, j], s_rs.at[a, j], device) for j, _, device in peers[a]
        ]
        stat_sends += sends
        for copy in sends:
            copy.start()
        sr_v[a, here[a]] = st_v[a]
        for copy in sends:
            copy.wait_recv()
        total = sum(sr_v[a, p] for p in range(ring))
        if a < 2:
            st_v[a + 1] = total

    c_g = beta * c_gate[...] + (1.0 - beta) * (total[0:1] / (rows * m))
    c_u = beta * c_up[...] + (1.0 - beta) * (total[2:3] / (rows * m))
    c_d = beta * c_down[...] + (1.0 - beta) * (total[4:5, :nd] / (rows * ma))
    c_gate_o[...] = c_g
    c_up_o[...] = c_u
    c_down_o[...] = c_d
    r_mean = [total[5:6, i * 128 : (i + 1) * 128] / (rows * size) for i, size in enumerate((m, m, ma))]
    ratio = (total[1:2] / c_g, total[3:4] / c_u, total[4:5, nd:] / c_d)
    for i in range(3):
        fs_v[i : i + 1, :] = jnp.sum(ratio[i], axis=1, keepdims=True) * r_mean[i]
        fs_v[i + 3 : i + 4, :] = total[6:7, i * 128 : (i + 1) * 128]
    fs_v[6:8, :] = jnp.zeros((2, 128), F32)
    last_swap = remote(fs_v, fr_v, e_ss, e_rs, partner)
    last_swap.start()
    scaled = []
    for g, r, c, mean in zip((g_g, g_u, g_d), wide, (c_g, c_u, c_d), r_mean, strict=True):
        scaled.append(g * lax.rsqrt(r * c / widen(mean, g.shape[1])))
    last_swap.wait_recv()
    sums = fs_v[...] + fr_v[...]
    for i, (w, out) in enumerate(((w_gate, w_gate_o), (w_up, w_up_o), (w_down, w_down_o))):
        count = rows * cores * w.shape[0] * w.shape[1]
        rms_u = jnp.sqrt(sums[i : i + 1] / count)
        rms_w = jnp.sqrt(sums[i + 3 : i + 4] / count)
        factor = rho * jnp.maximum(EPS_TWO, rms_w) / jnp.maximum(1.0, rms_u / bound)
        out[...] = w[...] - widen(factor, w.shape[1]) * scaled[i]

    for copy in own_sends:
        copy.wait_recv()
    for copy in dx_forwards:
        copy.wait_recv()
    for copy in own_copies:
        copy.wait()
    for copy in (*w_sends, *x_sends, *x_forwards, *part_sends, *dx_sends, *own_sends, *dx_forwards, *g_sends, *stat_sends):
        copy.wait_send()
    row_swap.wait_send()
    last_swap.wait_send()


def solution(mesh):
    row_size = mesh.shape["row"]
    cores = mesh.shape["col"]
    ring = round(row_size ** (1 / 3))
    weight_spec = P("row", "col")
    act_spec = P(None, "row")
    grad_spec = P(None, "col")
    in_specs = (weight_spec,) * 3 + (act_spec, act_spec) + (grad_spec,) * 3 + (P("row"), P("col")) * 3 + (P(),)
    out_specs = (weight_spec,) * 3 + (P("row"), P("col")) * 3 + (act_spec, act_spec)

    def body(w_gate, w_up, w_down, x_norm, x_act, dy_gate, dy_up, dy_down, r_gate, c_gate, r_up, c_up, r_down, c_down, hyper_params):
        tokens = x_norm.shape[0]
        m, nf = w_gate.shape
        ma, nd = w_down.shape
        th = tokens // ring // 2
        ah = th // 2
        n_ct = th // min(2048, th)
        peers = ring - 1
        dma = pltpu.SemaphoreType.DMA
        vmem = pl.BlockSpec(memory_space=pltpu.VMEM)
        anywhere = pl.BlockSpec(memory_space=pl.ANY)
        f32 = lambda *shape: jax.ShapeDtypeStruct(shape, F32)
        scratch = [
            pltpu.VMEM((2, th, nf), BF16), pltpu.VMEM((2, th, nf), BF16), pltpu.VMEM((2, ah, nd), BF16), pltpu.VMEM((2, ah, nd), BF16),
            pltpu.VMEM((ring, 2 * m, nf), BF16), pltpu.VMEM((ring, ma, nd), BF16), pltpu.VMEM((ring, ma, nd), BF16),
            pltpu.VMEM((ring * m, nf), BF16), pltpu.VMEM((ring * m, nf), BF16),
            pltpu.VMEM((2, ring, m, th), BF16), pltpu.VMEM((2, ring, ma, ah), BF16), pltpu.VMEM((2, ring, ma, ah), BF16),
            pltpu.VMEM((2, ring * m, th), BF16),
            *[pltpu.VMEM(shape, F32) for _ in range(3) for shape in ((ring * m, th), (ring * ma, ah), (ring * ma, ah))],
            pltpu.VMEM((ring, m, th), BF16), pltpu.VMEM((ring, ma, ah), BF16), pltpu.VMEM((ring, ma, ah), BF16),
            *[pltpu.VMEM(shape, F32) for _ in range(2) for shape in ((ring, 2 * m, nf), (ring, ma, nd), (ring, ma, nd))],
            pltpu.VMEM((2 * m + ma, 128), F32), pltpu.VMEM((2 * m + ma, 128), F32),
            pltpu.VMEM((3, 8, nf), F32), pltpu.VMEM((3, ring, 8, nf), F32),
            pltpu.VMEM((8, 128), F32), pltpu.VMEM((8, 128), F32),
            dma((2, n_ct)), dma((2, n_ct)), dma((2,)), dma((2,)), dma((3, 2)),
            *[dma((3, peers))] * 6, dma((3,)), dma((3,)), dma((3, peers)), dma((3, peers)),
            dma((3,)), dma((3,)), dma((3,)), dma((3, peers)), dma((3, peers)),
            dma((3, peers)), dma((3, peers)), dma, dma, dma((3, peers)), dma((3, peers)), dma, dma,
        ]
        outs = pl.pallas_call(
            functools.partial(step_kernel, (ring, cores, tokens)),
            out_shape=(
                f32(m, nf), f32(m, nf), f32(ma, nd), f32(1, m), f32(1, nf), f32(1, m), f32(1, nf), f32(1, ma), f32(1, nd),
                jax.ShapeDtypeStruct((m, tokens), BF16), jax.ShapeDtypeStruct((ma, tokens), BF16),
            ),
            in_specs=[pl.BlockSpec(memory_space=pltpu.SMEM)] + [vmem] * 3 + [anywhere] * 5 + [vmem] * 6,
            out_specs=(vmem,) * 9 + (anywhere,) * 2,
            scratch_shapes=scratch,
            compiler_params=pltpu.CompilerParams(collective_id=0, has_side_effects=True),
            name="adafactor_step",
        )(
            hyper_params, w_gate, w_up, w_down, x_norm.T, x_act.T, dy_gate, dy_up, dy_down,
            r_gate.reshape(1, -1), c_gate.reshape(1, -1), r_up.reshape(1, -1), c_up.reshape(1, -1),
            r_down.reshape(1, -1), c_down.reshape(1, -1),
        )
        new, stats, (dxn, dxa) = outs[:3], outs[3:9], outs[9:]
        return (*new, *(s.reshape(-1) for s in stats), dxn.T, dxa.T)

    return jax.shard_map(body, mesh=mesh, in_specs=in_specs, out_specs=out_specs, check_vma=False)
```

```python
import functools

import jax
import jax.numpy as jnp
from jax import lax
from jax.experimental import pallas as pl
from jax.experimental.pallas import tpu as pltpu
from jax.sharding import PartitionSpec as P

EPS_ONE = 1e-30
EPS_TWO = 1e-3
MESH = pl.DeviceIdType.MESH
BF16 = jnp.bfloat16
F32 = jnp.float32


def dot_nt(lhs, rhs):
    return lax.dot_general(lhs, rhs, (((1,), (1,)), ((), ())), preferred_element_type=F32)


def dot_nn(lhs, rhs):
    return lax.dot_general(lhs, rhs, (((1,), (0,)), ((), ())), preferred_element_type=F32)


def to_column(row_ref):
    m = row_ref.shape[1]
    eye = lax.broadcasted_iota(jnp.int32, (m, m), 0) == lax.broadcasted_iota(jnp.int32, (m, m), 1)
    spread = jnp.where(eye, jnp.broadcast_to(row_ref[...], (m, m)), 0.0)
    return jnp.broadcast_to(jnp.sum(spread, axis=1, keepdims=True), (m, 128))


def to_row(column):
    m = column.shape[0]
    eye = lax.broadcasted_iota(jnp.int32, (m, m), 0) == lax.broadcasted_iota(jnp.int32, (m, m), 1)
    return jnp.sum(jnp.where(eye, column[:, :m], 0.0), axis=0, keepdims=True)


def widen(column, n):
    return jnp.concatenate([column] * (n // 128), axis=1)


def step_kernel(
    dims,
    hyper_in, w_gate, w_up, w_down, xn, xa, dyg, dyu, dyd, r_gate, c_gate, r_up, c_up, r_down, c_down,
    w_gate_o, w_up_o, w_down_o, r_gate_o, c_gate_o, r_up_o, c_up_o, r_down_o, c_down_o, dxn_o, dxa_o,
    dyg_v, dyu_v, dya_v, dyb_v,
    wg_v, wu_v, wd_v, rg_v, cg_v, ru_v, cu_v, rd_v, cd_v, hyper,
    wn_v, wa_v, wb_v, wlg_v, wlu_v,
    xrn, xra, xrb, xln,
    dsn, dsa, dsb, dkn, dka, dkb, drn, dra, drb, fin_n, fin_a, fin_b,
    gpn, gpa, gpb, grn, gra, grb,
    st_v, sr_v, cc_v, res_v,
    ldg, ldu, lda, ldb, ldx, lds,
    w_ss, w_rs, x_ss, x_rs, xf_ss, xf_rs, p_ss, p_rs, d_ss, d_rs, o_ss, o_rs, f_ss, f_rs,
    g_ss, g_rs, y_ss, y_rs, s_ss, s_rs, c_ss, c_rs, e_ss, e_rs,
):
    ring, cores, tokens = dims
    m, nf = w_gate.shape
    ma, nd = w_down.shape
    tq = tokens // ring
    th = tq // 2
    aq = tq // 2
    ah = aq // 2
    ct = min(2048, th)
    n_ct = th // ct
    rows = ring**3
    chief = cores - 1

    core = lax.axis_index("col")
    row = lax.axis_index("row")
    partner = {"col": 1 - core}
    here, peers = [], []
    for stride in (1, ring, ring * ring):
        q = lax.rem(lax.div(row, stride), ring)
        here.append(q)
        group = []
        for k in range(1, ring):
            there = lax.rem(q + k, ring)
            group.append((k - 1, there, row + (there - q) * stride))
        peers.append(group)

    def remote(src, dst, send, recv, device):
        return pltpu.make_async_remote_copy(
            src_ref=src, dst_ref=dst, send_sem=send, recv_sem=recv, device_id=device, device_id_type=MESH
        )

    def half_of(s):
        return core if s else 1 - core

    bases = (0, 0, tokens // 2)
    shares = (tq, aq, aq)
    halves = (th, ah, ah)

    def token_start(axis, q, h):
        return pl.multiple_of(bases[axis] + q * shares[axis] + h * halves[axis], 128)

    def norm_load(src, dst, sem, s, i):
        start = pl.multiple_of(here[0] * tq + half_of(s) * th + i * ct, 128)
        return pltpu.make_async_copy(src.at[pl.ds(start, ct), :], dst.at[s, pl.ds(i * ct, ct), :], sem.at[s, i])

    def down_load(axis, dst, sem, s):
        start = token_start(axis, here[axis], half_of(s))
        return pltpu.make_async_copy(dyd.at[pl.ds(start, ah), :], dst.at[s], sem.at[s])

    x_src = (xn, xa, xa)
    x_dst = (xrn, xra, xrb)

    def x_piece(axis, q, h):
        return x_src[axis].at[:, pl.ds(token_start(axis, q, h), halves[axis])]

    barrier = pltpu.get_barrier_semaphore()
    pl.semaphore_signal(barrier, inc=1, device_id=partner, device_id_type=MESH)
    for group in peers:
        for _, _, device in group:
            pl.semaphore_signal(barrier, inc=1, device_id={"row": device}, device_id_type=MESH)

    small = [
        pltpu.make_async_copy(src, dst, lds.at[i])
        for i, (src, dst) in enumerate(
            ((w_gate, wg_v), (w_up, wu_v), (w_down, wd_v), (r_gate, rg_v), (c_gate, cg_v), (r_up, ru_v), (c_up, cu_v), (r_down, rd_v), (c_down, cd_v), (hyper_in, hyper))
        )
    ]
    for copy in small:
        copy.start()
    for copy in small:
        copy.wait()
    loads = []
    for s in (0, 1):
        group = []
        for i in range(n_ct):
            group += [norm_load(dyg, dyg_v, ldg, s, i), norm_load(dyu, dyu_v, ldu, s, i)]
        group += [down_load(1, dya_v, lda, s), down_load(2, dyb_v, ldb, s)]
        for copy in group:
            copy.start()
        loads.append(group)
    own_x = [
        pltpu.make_async_copy(x_piece(a, here[a], h), x_dst[a].at[h, here[a]], ldx.at[a, h])
        for a in range(3)
        for h in (0, 1)
    ]
    for copy in own_x:
        copy.start()

    wn_v[here[0]] = jnp.concatenate([wg_v[...], wu_v[...]], axis=0).astype(BF16)
    wa_v[here[1]] = wd_v[...].astype(BF16)
    wb_v[here[2]] = wd_v[...].astype(BF16)
    cc_v[0] = jnp.zeros(cc_v.shape[1:], F32)
    cc_v[0, 0:1, :] = cg_v[...]
    cc_v[0, 1:2, :] = cu_v[...]
    cc_v[0, 2:3, :nd] = cd_v[...]
    for i, w in enumerate((wg_v, wu_v, wd_v)):
        cc_v[0, 3:4, i * 128 : (i + 1) * 128] = jnp.broadcast_to(jnp.sum(w[...] * w[...]).reshape(1, 1), (1, 128))

    pl.semaphore_wait(barrier, 1 + 3 * (ring - 1))

    w_bufs = (wn_v, wa_v, wb_v)
    w_sends, x_sends = [], []
    for a in range(3):
        for j, there, device in peers[a]:
            slot = w_bufs[a].at[here[a]]
            w_sends.append(remote(slot, slot, w_ss.at[a, j], w_rs.at[a, j], {"row": device}))
    for j in range(ring - 1):
        for a in range(3):
            _, there, device = peers[a][j]
            x_sends.append(
                remote(x_piece(a, there, core), x_dst[a].at[core, here[a]], x_ss.at[a, j], x_rs.at[a, j], {"row": device})
            )
    for copy in w_sends:
        copy.start()
    for copy in x_sends:
        copy.start()

    for copy in w_sends:
        copy.wait_recv()
    stacked = [wn_v[p].astype(F32) for p in range(ring)]
    wlg_v[...] = jnp.concatenate([v[:m] for v in stacked], axis=0).astype(BF16)
    wlu_v[...] = jnp.concatenate([v[m:] for v in stacked], axis=0).astype(BF16)

    cc_send = remote(cc_v.at[0], cc_v.at[1], c_ss, c_rs, partner)

    @pl.when(core != chief)
    def _():
        cc_send.start()

    def dx_norm(s, out):
        for i in range(n_ct):
            part = slice(i * ct, (i + 1) * ct)
            out[:, part] = dot_nt(wlg_v[...], dyg_v[s, part, :]) + dot_nt(wlu_v[...], dyu_v[s, part, :])

    def dx_down(s, dy_v, w_v, out):
        out[...] = dot_nt(w_v[...].reshape(ring * ma, nd), dy_v[s])

    part_sends = [
        remote(src, dst, p_ss.at[a], p_rs.at[a], partner) for a, (src, dst) in enumerate(((dsn, drn), (dsa, dra), (dsb, drb)))
    ]
    for copy in loads[0]:
        copy.wait()
    dx_norm(0, dsn)
    dx_down(0, dya_v, wa_v, dsa)
    dx_down(0, dyb_v, wb_v, dsb)
    for copy in part_sends:
        copy.start()
    for copy in loads[1]:
        copy.wait()

    dx_out = (dxn_o, dxa_o, dxa_o)
    fins = (fin_n, fin_a, fin_b)

    def out_piece(axis, q, h):
        return dx_out[axis].at[:, pl.ds(token_start(axis, q, h), halves[axis])]

    dx_sends, own_sends = [], []
    for a in range(3):
        target = out_piece(a, here[a], core)
        own_sends.append(remote(target, target, o_ss.at[a], o_rs.at[a], partner))
        for j, there, device in peers[a]:
            dx_sends.append(remote(fins[a].at[there], target, d_ss.at[a, j], d_rs.at[a, j], {"row": device}))

    def finish(a, kept, got):
        part_sends[a].wait_recv()
        total = (kept[...] + got[...]).astype(BF16)
        size = fins[a].shape[1]
        for p in range(ring):
            fins[a][p] = total[p * size : (p + 1) * size]
        dx_out[a][:, pl.ds(token_start(a, here[a], core), halves[a])] = fins[a][here[a]]
        for copy in dx_sends[a * (ring - 1) : (a + 1) * (ring - 1)]:
            copy.start()
        own_sends[a].start()

    dx_norm(1, dkn)
    finish(0, dkn, drn)

    x_forwards = []
    for j in range(ring - 1):
        for a in range(3):
            origin = lax.rem(here[a] + ring - (j + 1), ring)
            slot = x_dst[a].at[core, origin]
            x_forwards.append(remote(slot, slot, xf_ss.at[a, j], xf_rs.at[a, j], partner))
    for got, forward in zip(x_sends, x_forwards, strict=True):
        got.wait_recv()
        forward.start()
    for copy in own_x:
        copy.wait()

    def grads_of(s):
        h = half_of(s)
        xln[s] = jnp.concatenate([xrn[h, p].astype(F32) for p in range(ring)], axis=0).astype(BF16)
        return (
            dot_nn(xln[s], dyg_v[s]),
            dot_nn(xln[s], dyu_v[s]),
            dot_nn(xra[h].reshape(ring * ma, ah), dya_v[s]),
            dot_nn(xrb[h].reshape(ring * ma, ah), dyb_v[s]),
        )

    def put_grads(values, add):
        g_g, g_u, g_a, g_b = values
        for p in range(ring):
            for i, g in enumerate((g_g, g_u)):
                piece = g[p * m : (p + 1) * m]
                gpn[p, i * m : (i + 1) * m, :] = gpn[p, i * m : (i + 1) * m, :] + piece if add else piece
        for out, g in ((gpa, g_a), (gpb, g_b)):
            g = g.reshape(ring, ma, nd)
            out[...] = out[...] + g if add else g

    put_grads(grads_of(1), False)

    for forward in x_forwards:
        forward.wait_recv()

    put_grads(grads_of(0), True)

    g_bufs = ((gpn, grn), (gpa, gra), (gpb, grb))
    g_sends = [
        remote(src.at[there], dst.at[core, here[a]], g_ss.at[a, j], g_rs.at[core, a, j], {"row": device, "col": chief})
        for a, (src, dst) in enumerate(g_bufs)
        for j, there, device in peers[a]
    ]
    y_sends = [
        remote(src.at[here[a]], dst.at[core, here[a]], y_ss.at[a], y_rs.at[a], partner) for a, (src, dst) in enumerate(g_bufs)
    ]
    for copy in g_sends:
        copy.start()

    @pl.when(core != chief)
    def _():
        for copy in y_sends:
            copy.start()

    @pl.when(core == chief)
    def _():
        for a, (src, dst) in enumerate(g_bufs):
            dst[chief, here[a]] = src[here[a]]

    dx_down(1, dya_v, wa_v, dka)
    dx_down(1, dyb_v, wb_v, dkb)
    finish(1, dka, dra)
    finish(2, dkb, drb)

    dx_forwards = []
    for a in range(3):
        for j, _, _ in peers[a]:
            origin = lax.rem(here[a] + ring - (j + 1), ring)
            piece = out_piece(a, origin, core)
            dx_forwards.append(remote(piece, piece, f_ss.at[a, j], f_rs.at[a, j], partner))

    def forward_dx(axes):
        for a in axes:
            for j in range(ring - 1):
                dx_sends[a * (ring - 1) + j].wait_recv()
                dx_forwards[a * (ring - 1) + j].start()

    res_send = remote(res_v, res_v, e_ss, e_rs, partner)
    stat_sends = [
        [remote(st_v.at[a], sr_v.at[a, here[a]], s_ss.at[a, j], s_rs.at[a, j], {"row": device}) for j, _, device in peers[a]]
        for a in range(3)
    ]
    down_row = 2 * m
    last_row = 2 * m + ma

    @pl.when(core != chief)
    def _():
        forward_dx((0, 1, 2))
        res_send.wait_recv()
        w_gate_o[...] = wg_v[...] - res_v[0:m, :]
        w_up_o[...] = wu_v[...] - res_v[m : 2 * m, :]
        w_down_o[...] = wd_v[...] - res_v[down_row:last_row, :nd]
        c_gate_o[...] = res_v[last_row : last_row + 1, :]
        c_up_o[...] = res_v[last_row + 1 : last_row + 2, :]
        c_down_o[...] = res_v[last_row + 2 : last_row + 3, :nd]
        r_gate_o[...] = res_v[last_row + 3 : last_row + 4, 0:m]
        r_up_o[...] = res_v[last_row + 3 : last_row + 4, 128 : 128 + m]
        r_down_o[...] = res_v[last_row + 3 : last_row + 4, 256 : 256 + ma]
        for copies in (y_sends, [cc_send]):
            for copy in copies:
                copy.wait_send()

    @pl.when(core == chief)
    def _():
        beta = hyper[0]
        rho = hyper[1]
        bound = hyper[2]
        rc_g, rc_u, rc_d = to_column(rg_v), to_column(ru_v), to_column(rd_v)
        res_v[last_row:, :] = jnp.zeros((8, nf), F32)
        cc_send.wait_recv()
        for c in range(cores):
            for a, (src, dst) in enumerate(g_bufs):
                for j in range(ring - 1):
                    remote(src.at[0], dst.at[c, 0], g_ss.at[a, j], g_rs.at[c, a, j], partner).wait_recv()
        for copy in y_sends:
            copy.wait_recv()
        grad = []
        for c in range(cores):
            g_n = sum(grn[c, p] for p in range(ring))
            grad.append((g_n[:m], g_n[m:], sum(gra[c, p] for p in range(ring)) + sum(grb[c, p] for p in range(ring))))
        sq = [[g * g for g in gs] for gs in grad]
        sizes = (m, m, ma)
        lanes = (nf, nf, nd)
        r_new, wide = [], []
        for i, r_old in enumerate((rc_g, rc_u, rc_d)):
            row_sum = sum(jnp.sum(sq[c][i] + EPS_ONE, axis=1, keepdims=True) for c in range(cores))
            row_mean = jnp.broadcast_to(row_sum, (sizes[i], 128)) / (cores * lanes[i])
            r_new.append(beta * r_old + (1.0 - beta) * row_mean)
            wide.append(widen(r_new[i], lanes[i]))

        st_v[0] = jnp.zeros(st_v.shape[1:], F32)
        for i in range(3):
            inverse = 1.0 / wide[i]
            for c in range(cores):
                q_sum = jnp.sum(sq[c][i] + EPS_ONE, axis=0, keepdims=True)
                u_sum = jnp.sum(sq[c][i] * inverse, axis=0, keepdims=True)
                if i < 2:
                    st_v[0, 8 * c + 2 * i : 8 * c + 2 * i + 1, :] = q_sum
                    st_v[0, 8 * c + 2 * i + 1 : 8 * c + 2 * i + 2, :] = u_sum
                else:
                    st_v[0, 8 * c + 4 : 8 * c + 5, :nd] = q_sum
                    st_v[0, 8 * c + 4 : 8 * c + 5, nd:] = u_sum
            st_v[0, 5:6, i * 128 : (i + 1) * 128] = jnp.sum(r_new[i], axis=0, keepdims=True)
        st_v[0, 6:7, :] = cc_v[0, 3:4, :] + cc_v[1, 3:4, :]
        total = None
        for a in range(3):
            for copy in stat_sends[a]:
                copy.start()
            sr_v[a, here[a]] = st_v[a]
            if a == 0:
                for i, (r, out) in enumerate(zip(r_new, (r_gate_o, r_up_o, r_down_o), strict=True)):
                    line = to_row(r)
                    out[...] = line
                    res_v[last_row + 3 : last_row + 4, i * 128 : i * 128 + sizes[i]] = line
            forward_dx(((0,), (1, 2), ())[a])
            for copy in stat_sends[a]:
                copy.wait_recv()
            total = sum(sr_v[a, p] for p in range(ring))
            if a < 2:
                st_v[a + 1] = total

        r_mean = [total[5:6, i * 128 : (i + 1) * 128] / (rows * sizes[i]) for i in range(3)]
        factor = []
        c_new = [[], []]
        for i in range(3):
            u_sq = 0.0
            for c in range(cores):
                base = 8 * c
                if i < 2:
                    q_sum = total[base + 2 * i : base + 2 * i + 1]
                    u_sum = total[base + 2 * i + 1 : base + 2 * i + 2]
                else:
                    q_sum = total[base + 4 : base + 5, :nd]
                    u_sum = total[base + 4 : base + 5, nd:]
                c_old = cc_v[0 if c == chief else 1, i : i + 1, : lanes[i]]
                c_new[c].append(beta * c_old + (1.0 - beta) * (q_sum / (rows * sizes[i])))
                u_sq += jnp.sum(u_sum / c_new[c][i], axis=1, keepdims=True)
            count = rows * cores * sizes[i] * lanes[i]
            rms_u = jnp.sqrt(u_sq * r_mean[i] / count)
            rms_w = jnp.sqrt(total[6:7, i * 128 : (i + 1) * 128] / count)
            factor.append(rho * jnp.maximum(EPS_TWO, rms_w) / jnp.maximum(1.0, rms_u / bound))
        for c in range(cores):
            step = []
            for i in range(3):
                v = wide[i] * c_new[c][i] / widen(r_mean[i], lanes[i])
                step.append(widen(factor[i], lanes[i]) * (grad[c][i] * lax.rsqrt(v)))
            if c != chief:
                res_v[0:m, :] = step[0]
                res_v[m : 2 * m, :] = step[1]
                res_v[down_row:last_row, :nd] = step[2]
                res_v[last_row : last_row + 1, :] = c_new[c][0]
                res_v[last_row + 1 : last_row + 2, :] = c_new[c][1]
                res_v[last_row + 2 : last_row + 3, :nd] = c_new[c][2]
                res_send.start()
            else:
                for i, (w, out) in enumerate(((wg_v, w_gate_o), (wu_v, w_up_o), (wd_v, w_down_o))):
                    out[...] = w[...] - step[i]
                for i, out in enumerate((c_gate_o, c_up_o, c_down_o)):
                    out[...] = c_new[c][i]
        for sends in (*stat_sends, [res_send]):
            for copy in sends:
                copy.wait_send()

    for copy in own_sends:
        copy.wait_recv()
    for copy in dx_forwards:
        copy.wait_recv()
    for copy in (*w_sends, *x_sends, *x_forwards, *part_sends, *dx_sends, *own_sends, *dx_forwards, *g_sends):
        copy.wait_send()


def write_kernel(*refs):
    count = (len(refs) - 1) // 2
    sems = refs[-1]
    copies = [pltpu.make_async_copy(refs[i], refs[count + i], sems.at[i]) for i in range(count)]
    for copy in reversed(copies):
        copy.start()
    for copy in copies:
        copy.wait()


def solution(mesh):
    row_size = mesh.shape["row"]
    cores = mesh.shape["col"]
    ring = round(row_size ** (1 / 3))
    weight_spec = P("row", "col")
    act_spec = P(None, "row")
    grad_spec = P(None, "col")
    in_specs = (weight_spec,) * 3 + (act_spec, act_spec) + (grad_spec,) * 3 + (P("row"), P("col")) * 3 + (P(),)
    out_specs = (weight_spec,) * 3 + (P("row"), P("col")) * 3 + (act_spec, act_spec)

    def body(w_gate, w_up, w_down, x_norm, x_act, dy_gate, dy_up, dy_down, r_gate, c_gate, r_up, c_up, r_down, c_down, hyper_params):
        tokens = x_norm.shape[0]
        m, nf = w_gate.shape
        ma, nd = w_down.shape
        th = tokens // ring // 2
        ah = th // 2
        n_ct = th // min(2048, th)
        peers = ring - 1
        dma = pltpu.SemaphoreType.DMA
        vmem = pl.BlockSpec(memory_space=pltpu.VMEM)
        anywhere = pl.BlockSpec(memory_space=pltpu.HBM)
        scratch = [
            pltpu.VMEM((2, th, nf), BF16), pltpu.VMEM((2, th, nf), BF16), pltpu.VMEM((2, ah, nd), BF16), pltpu.VMEM((2, ah, nd), BF16),
            *[pltpu.VMEM(s, F32) for s in ((m, nf), (m, nf), (ma, nd), (1, m), (1, nf), (1, m), (1, nf), (1, ma), (1, nd))],
            pltpu.SMEM((3,), F32),
            pltpu.VMEM((ring, 2 * m, nf), BF16), pltpu.VMEM((ring, ma, nd), BF16), pltpu.VMEM((ring, ma, nd), BF16),
            pltpu.VMEM((ring * m, nf), BF16), pltpu.VMEM((ring * m, nf), BF16),
            pltpu.VMEM((2, ring, m, th), BF16), pltpu.VMEM((2, ring, ma, ah), BF16), pltpu.VMEM((2, ring, ma, ah), BF16),
            pltpu.VMEM((2, ring * m, th), BF16),
            *[pltpu.VMEM(shape, F32) for _ in range(3) for shape in ((ring * m, th), (ring * ma, ah), (ring * ma, ah))],
            pltpu.VMEM((ring, m, th), BF16), pltpu.VMEM((ring, ma, ah), BF16), pltpu.VMEM((ring, ma, ah), BF16),
            *[pltpu.VMEM(s, F32) for s in ((ring, 2 * m, nf), (ring, ma, nd), (ring, ma, nd))],
            *[pltpu.VMEM((cores, *s), F32) for s in ((ring, 2 * m, nf), (ring, ma, nd), (ring, ma, nd))],
            pltpu.VMEM((3, 8 * cores, nf), F32), pltpu.VMEM((3, ring, 8 * cores, nf), F32),
            pltpu.VMEM((2, 8, nf), F32), pltpu.VMEM((2 * m + ma + 8, nf), F32),
            dma((2, n_ct)), dma((2, n_ct)), dma((2,)), dma((2,)), dma((3, 2)), dma((10,)),
            *[dma((3, peers))] * 6, dma((3,)), dma((3,)), dma((3, peers)), dma((3, peers)),
            dma((3,)), dma((3,)), dma((3, peers)), dma((3, peers)),
            dma((3, peers)), dma((cores, 3, peers)), dma((3,)), dma((3,)), dma((3, peers)), dma((3, peers)), dma, dma, dma, dma,
        ]
        shapes = [(s, F32) for s in ((m, nf), (m, nf), (ma, nd), (1, m), (1, nf), (1, m), (1, nf), (1, ma), (1, nd))]
        shapes += [((m, tokens), BF16), ((ma, tokens), BF16)]
        operands = (
            hyper_params, w_gate, w_up, w_down, x_norm.T, x_act.T, dy_gate, dy_up, dy_down,
            r_gate.reshape(1, -1), c_gate.reshape(1, -1), r_up.reshape(1, -1), c_up.reshape(1, -1),
            r_down.reshape(1, -1), c_down.reshape(1, -1),
        )
        held = pl.pallas_call(
            functools.partial(step_kernel, (ring, cores, tokens)),
            out_shape=tuple(pltpu.VMEM(s, d) for s, d in shapes),
            in_specs=[anywhere] * 15,
            out_specs=(vmem,) * len(shapes),
            scratch_shapes=scratch,
            compiler_params=pltpu.CompilerParams(collective_id=0, has_side_effects=True, vmem_limit_bytes=48 * 2**20),
            name="adafactor_step",
        )(*[pltpu.with_memory_space_constraint(v, pltpu.HBM) for v in operands])
        outs = pl.pallas_call(
            write_kernel,
            out_shape=tuple(jax.ShapeDtypeStruct(s, d) for s, d in shapes),
            in_specs=[vmem] * len(shapes),
            out_specs=(anywhere,) * len(shapes),
            scratch_shapes=[dma((len(shapes),))],
            compiler_params=pltpu.CompilerParams(vmem_limit_bytes=4 * 2**20),
            name="write_results",
        )(*held)
        new, stats, (dxn, dxa) = outs[:3], outs[3:9], outs[9:]
        return (*new, *(s.reshape(-1) for s in stats), dxn.T, dxa.T)

    return jax.shard_map(body, mesh=mesh, in_specs=in_specs, out_specs=out_specs, check_vma=False)
```
